512 devices in a mesh: snap: 32 (over z, x_hi, core), space: 16 (over y, x_lo).
Axes of the slice: x: 4 (x_hi: 2, x_lo: 2; x = x_hi * 2 + x_lo), y: 8, z: 8, core: 2. Of those that a mesh axis runs over, the one named last changes fastest.
Arguments:
- snapshots: bfloat16 [65536, 4096], P('space', 'snap'), may hold values from -36 to 36
Outputs:
- gram_band: float32 [4096, 2176], P(('snap', 'space'))
- mean_field: float32 [65536], P('space')
The draws below stay inside these ranges and needn't reach their ends.
All inputs are finite; a program needn't handle non-finite values.
Results may differ from the reference program's by a relative error of at most 0.00036.
Values may be sent and summed in bfloat16 or wider, within the bound.
A program may use at most 64 MiB of HBM per device.

```python
import jax
import jax.numpy as jnp
from jax import lax

SNAP_DEV = 128
ROWS = 65536
SNAPS = 4096
N_SNAP = 32


def draw_snapshots(key, part):
    key_level, key_scale, key_noise = jax.random.split(jax.random.fold_in(key, 17), 3)
    level = jnp.clip(jax.random.normal(key_level, (ROWS, 1), jnp.float32), -4.0, 4.0)
    moments = jnp.arange(SNAPS, dtype=jnp.float32)[None, :] / SNAPS
    ramp_values = 0.5 + moments
    row_scale = jnp.exp(jax.random.uniform(key_scale, (ROWS, 1), jnp.float32, jnp.log(0.3), jnp.log(3.0)))
    noise_values = jnp.clip(jax.random.normal(key_noise, (ROWS, SNAPS), jnp.float32), -4.0, 4.0)
    values = row_scale * (level * ramp_values + ramp_values * noise_values)
    return values.astype(jnp.bfloat16)


def setup_inputs(seed: int = 0) -> dict:
    key_list = jax.random.split(jax.random.key(seed), 2)
    snapshots = draw_snapshots(jax.random.fold_in(key_list[1], 71), 0)
    return dict(snapshots=snapshots)


def reference(snapshots):
    mean_field = jnp.sum(snapshots.astype(jnp.float32), axis=1) / SNAPS
    fluctuation = (snapshots.astype(jnp.float32) - mean_field[:, None]).astype(jnp.bfloat16)
    band_blocks = N_SNAP // 2 + 1
    extended = jnp.concatenate([fluctuation, fluctuation[:, :band_blocks * SNAP_DEV]], axis=1)

    def one_row(block_index):
        first_col = (block_index * SNAP_DEV).astype(jnp.int32)
        own_block = lax.dynamic_slice_in_dim(fluctuation, first_col, SNAP_DEV, 1)
        window = lax.dynamic_slice_in_dim(extended, first_col, band_blocks * SNAP_DEV, 1)
        return jnp.dot(own_block.T, window, preferred_element_type=jnp.float32)

    rows_out = lax.map(one_row, jnp.arange(N_SNAP, dtype=jnp.int32))
    gram_band = rows_out.reshape(SNAPS, band_blocks * SNAP_DEV) * (1.0 / ROWS)
    return gram_band, mean_field
```

```python
import jax
import jax.numpy as jnp
from jax import lax
from jax.experimental import pallas as pl
from jax.experimental.pallas import tpu as pltpu
from jax.sharding import PartitionSpec as P

MESH = pl.DeviceIdType.MESH
NZ, NX, NY = 8, 4, 8
LANES = 128
ROWS_Q = 1024
SNAPS = 4096
ROWS = 65536
GROUPS = 10
F32, BF16 = jnp.float32, jnp.bfloat16


def device(z, x, y, c):
    z, x, y = (z + NZ) % NZ, (x + NX) % NX, (y + NY) % NY
    return (z * 4 + (x // 2) * 2 + c, y * 2 + x % 2)


def wait_for(ref, sem):
    pltpu.make_async_copy(ref, ref, sem).wait()


def kernel(
    a_ref, gram_ref, mean_ref,
    raw0, lo1, hi1, lo2, hi2, lhs, mcol, psum, qrecv, zrecv, mall,
    part, drecv, xbuf, xrecv, ybuf, yrecv,
    quad_s, quad_r, psum_s, psum_r, zsum_s, zsum_r, mean_s, mean_r,
    up1_s, up1_r, dn1_s, dn1_r, up2_s, up2_r, dn2_s, dn2_r,
    d_s, d_r, x_s, x_r, y_s, y_r,
):
    s, p = lax.axis_index("snap"), lax.axis_index("space")
    z, xh, c = s // 4, (s // 2) % 2, s % 2
    y, xl = p // 2, p % 2
    x = xh * 2 + xl
    q0 = xh * 2 + c
    quad = {
        1: (device(z, x, y, 1 - c), xh * 2 + 1 - c),
        2: (device(z, x + 2, y, c), (1 - xh) * 2 + c),
        3: (device(z, x + 2, y, 1 - c), (1 - xh) * 2 + 1 - c),
    }

    def send(src, dst, ss, rs, to):
        pltpu.make_async_remote_copy(
            src_ref=src, dst_ref=dst, send_sem=ss, recv_sem=rs,
            device_id=to, device_id_type=MESH,
        ).start()

    barrier = pltpu.get_barrier_semaphore()
    sources = [device(z - k, x, y, c) for k in range(1, NZ)]
    sources += [quad[1][0], quad[2][0], quad[3][0]]
    sources += [device(z, x + 1, y, c), device(z, x + 3, y, c)]
    for shift in range(3):
        sources += [device(z + shift, x, y - k, c) for k in range(1, NY)]
    for to in sources:
        pl.semaphore_signal(barrier, inc=1, device_id=to, device_id_type=MESH)

    def row_sums(i, carry):
        block = a_ref[pl.ds(pl.multiple_of(i * LANES, LANES), LANES), :].astype(F32)
        psum[pl.ds(i, 1), :] = jnp.sum(block.T, axis=0, keepdims=True)
        return carry

    lax.fori_loop(0, 32, row_sums, 0)
    own_rows = pl.ds(pl.multiple_of(q0 * ROWS_Q, ROWS_Q), ROWS_Q)
    raw0[q0] = a_ref[own_rows, :]

    pl.semaphore_wait(barrier, len(sources))

    for j in (1, 2, 3):
        to, q = quad[j]
        send(psum.at[pl.ds(pl.multiple_of(q * 8, 8), 8)], qrecv.at[j - 1], psum_s, psum_r, to)

    above, below = device(z + 1, x, y, c), device(z - 1, x, y, c)

    def send_slab(src, a):
        send(src, lo1.at[a], up1_s.at[a], up1_r.at[a], above)
        send(src, hi1.at[a], dn1_s.at[a], dn1_r.at[a], below)

    send_slab(a_ref.at[own_rows], q0)
    for j in (1, 2, 3):
        to, q = quad[j]
        rows = pl.ds(pl.multiple_of(q * ROWS_Q, ROWS_Q), ROWS_Q)
        send(a_ref.at[rows], raw0.at[q0], quad_s.at[j - 1], quad_r.at[j - 1], to)

    wait_for(qrecv, psum_r)
    zrecv[z] = psum[pl.ds(pl.multiple_of(q0 * 8, 8), 8), :] + qrecv[0] + qrecv[1] + qrecv[2]
    for k in range(1, NZ):
        send(zrecv.at[z], zrecv.at[z], zsum_s, zsum_r, device(z + k, x, y, c))

    def quad_slab(j):
        q = quad[j][1]
        wait_for(raw0.at[q], quad_r.at[j - 1])
        send_slab(raw0.at[q], q)

    quad_slab(1)
    quad_slab(2)

    wait_for(zrecv.at[pl.ds(0, NZ - 1)], zsum_r)
    mean = zrecv[0]
    for k in range(1, NZ):
        mean = mean + zrecv[k]
    mean = mean * (1.0 / SNAPS)
    mall[q0] = mean
    for j in (1, 2, 3):
        send(mall.at[q0], mall.at[q0], mean_s, mean_r, quad[j][0])
    for g in range(8):
        mcol[pl.ds(g * LANES, LANES), :] = jnp.broadcast_to(mean[g : g + 1, :], (LANES, LANES)).T

    quad_slab(3)

    def centred(ref, a):
        return (ref[a].astype(F32) - mcol[...]).astype(BF16)

    def fill_lhs(ref, a, at):
        lhs[pl.ds(at * 512 + a * LANES, LANES), :] = centred(ref, a).T

    def store_unit(g, u, tile, first=0):
        blocks = tile.reshape((4 - first), 8, 2, 8, LANES)
        for a in range(4):
            for half in range(2):
                if a < first:
                    value = jnp.zeros((8, 8, LANES), F32)
                else:
                    value = blocks[a - first, :, half]
                part[g, a % 2, (a // 2) * 2 + half, u] = value

    def dot(start, size, right):
        return jnp.dot(lhs[pl.ds(start, size), :], right, preferred_element_type=F32)

    groups = [("a", 3), ("a", 1)] + [("b", t) for t in (3, 2, 1, 0)] + [("c", t) for t in (3, 2, 1, 0)]
    shifts = {"a": (0, 0), "b": (0, 1), "c": (1, 2)}
    dz = {"a": (0, 0), "b": (1, 2), "c": (3, 4)}

    def make(g):
        kind, t = groups[g]
        if kind == "a":
            for u in range(2):
                store_unit(g, u, dot(0, 512, centred(raw0, t - u)))
        elif kind == "b":
            right = centred(hi1, t)
            for u in range(2):
                store_unit(g, u, dot(u * 512, 512, right))
        else:
            wait_for(lo2.at[t], up2_r.at[t])
            wait_for(hi2.at[t], dn2_r.at[t])
            fill_lhs(lo2, t, 2)
            right = centred(hi2, t)
            store_unit(g, 0, dot(512, 512, right))
            store_unit(g, 1, dot(1024 + t * LANES, 512 - t * LANES, right), t)
        send(part.at[g, 1 - c], drecv.at[g], d_s.at[g], d_r.at[g], quad[1][0])

    def x_step(g):
        wait_for(drecv.at[g], d_r.at[g])
        xbuf[g] = part[g, c] + drecv[g]
        for k in range(1, NX):
            xt = (x + k) % NX
            send(xbuf.at[g, xt], xrecv.at[g, k - 1], x_s.at[g], x_r.at[g], device(z, xt, y, c))

    def y_step(g):
        wait_for(xrecv.at[g], x_r.at[g])
        ybuf[g] = xbuf[g, x] + xrecv[g, 0] + xrecv[g, 1] + xrecv[g, 2]
        for u in range(2):
            shift = shifts[groups[g][0]][u]
            for k in range(0 if shift else 1, NY):
                yt = (y + k) % NY
                send(ybuf.at[g, u, yt], yrecv.at[g, u, k], y_s.at[g, u], y_r.at[g, u], device(z - shift, x, yt, c))

    def o_step(g):
        kind, t = groups[g]
        for u in range(2):
            first = 0 if shifts[kind][u] else 1
            wait_for(yrecv.at[g, u, pl.ds(first, NY - first)], y_r.at[g, u])
            total = yrecv[g, u, 0] if first == 0 else ybuf[g, u, y]
            for k in range(1, NY):
                total = total + yrecv[g, u, k]
            total = total * (1.0 / ROWS)
            d = dz[kind][u]
            col = t - u if kind == "a" else t

            def put(total=total, d=d, col=col):
                at = pl.multiple_of((4 * d + col - q0) * LANES, LANES)
                gram_ref[:, pl.ds(at, LANES)] = total

            if d == 0:
                pl.when(col >= q0)(put)
            elif d == 4:
                pl.when(col <= q0)(put)
            else:
                put()

    for a in range(4):
        fill_lhs(raw0, a, 0)
    make(0)
    make(1)
    x_step(0)
    for t in (3, 2, 1, 0):
        wait_for(lo1.at[t], up1_r.at[t])
        send(lo1.at[t], lo2.at[t], up2_s.at[t], up2_r.at[t], above)
        wait_for(hi1.at[t], dn1_r.at[t])
        send(hi1.at[t], hi2.at[t], dn2_s.at[t], dn2_r.at[t], below)
    x_step(1)
    for t in (3, 2, 1, 0):
        fill_lhs(lo1, t, 1)
    for g in range(2, GROUPS):
        make(g)
        if g > 2:
            x_step(g - 1)
        y_step(g - 2)
        if g > 2:
            o_step(g - 3)
    x_step(GROUPS - 1)
    y_step(GROUPS - 2)
    o_step(GROUPS - 3)
    y_step(GROUPS - 1)
    o_step(GROUPS - 2)
    o_step(GROUPS - 1)

    wait_for(mall.at[pl.ds(0, 3)], mean_r)
    mean_ref[...] = mall[...]

    wait_for(qrecv, psum_s)
    wait_for(zrecv.at[pl.ds(0, NZ - 1)], zsum_s)
    wait_for(mall.at[pl.ds(0, 3)], mean_s)
    for j in range(3):
        wait_for(raw0.at[j], quad_s.at[j])
    for a in range(4):
        for sem in (up1_s, dn1_s, up2_s, dn2_s):
            wait_for(raw0.at[a], sem.at[a])
    for g in range(GROUPS):
        wait_for(drecv.at[g], d_s.at[g])
        wait_for(xrecv.at[g], x_s.at[g])
        for u in range(2):
            first = 0 if shifts[groups[g][0]][u] else 1
            wait_for(yrecv.at[g, u, pl.ds(first, NY - first)], y_s.at[g, u])


def per_device(snapshots):
    slab = lambda: pltpu.VMEM((4, ROWS_Q, LANES), BF16)
    dma = pltpu.SemaphoreType.DMA
    one = lambda: dma(())
    gram, mean = pl.pallas_call(
        kernel,
        out_shape=(
            jax.ShapeDtypeStruct((8, 17 * LANES), F32),
            jax.ShapeDtypeStruct((4, 8, LANES), F32),
        ),
        in_specs=[pl.BlockSpec(memory_space=pltpu.VMEM)],
        out_specs=(pl.BlockSpec(memory_space=pltpu.VMEM),) * 2,
        scratch_shapes=[
            slab(), slab(), slab(), slab(), slab(),
            pltpu.VMEM((3 * 512, ROWS_Q), BF16),
            pltpu.VMEM((ROWS_Q, LANES), F32),
            pltpu.VMEM((32, LANES), F32),
            pltpu.VMEM((3, 8, LANES), F32),
            pltpu.VMEM((NZ, 8, LANES), F32),
            pltpu.VMEM((4, 8, LANES), F32),
            pltpu.VMEM((GROUPS, 2, NX, 2, NY, 8, LANES), F32),
            pltpu.VMEM((GROUPS, NX, 2, NY, 8, LANES), F32),
            pltpu.VMEM((GROUPS, NX, 2, NY, 8, LANES), F32),
            pltpu.VMEM((GROUPS, NX - 1, 2, NY, 8, LANES), F32),
            pltpu.VMEM((GROUPS, 2, NY, 8, LANES), F32),
            pltpu.VMEM((GROUPS, 2, NY, 8, LANES), F32),
            dma((3,)), dma((3,)), one(), one(), one(), one(), one(), one(),
            dma((4,)), dma((4,)), dma((4,)), dma((4,)), dma((4,)), dma((4,)), dma((4,)), dma((4,)),
            dma((GROUPS,)), dma((GROUPS,)), dma((GROUPS,)), dma((GROUPS,)),
            dma((GROUPS, 2)), dma((GROUPS, 2)),
        ],
        compiler_params=pltpu.CompilerParams(
            collective_id=0, has_side_effects=True, vmem_limit_bytes=48 * 1024 * 1024
        ),
    )(snapshots)
    return gram, mean.reshape(-1)


def solution(mesh):
    return jax.shard_map(
        per_device,
        mesh=mesh,
        in_specs=(P("space", "snap"),),
        out_specs=(P(("snap", "space"), None), P("space")),
        check_vma=False,
    )
```

```python
import jax
import jax.numpy as jnp
from jax import lax
from jax.experimental import pallas as pl
from jax.experimental.pallas import tpu as pltpu
from jax.sharding import PartitionSpec as P

MESH = pl.DeviceIdType.MESH
NZ, NX, NY = 8, 4, 8
LANES = 128
ROWS_Q = 1024
SNAPS = 4096
ROWS = 65536
GROUPS = 10
F32, BF16 = jnp.float32, jnp.bfloat16


def device(z, x, y, c):
    z, x, y = (z + NZ) % NZ, (x + NX) % NX, (y + NY) % NY
    return (z * 4 + (x // 2) * 2 + c, y * 2 + x % 2)


def wait_for(ref, sem):
    pltpu.make_async_copy(ref, ref, sem).wait()


def kernel(
    a_ref, gram_ref, mean_ref,
    raw0, lo1, hi1, lo2, hi2, lhs, mcol, psum, qrecv, zrecv, mall,
    part, drecv, xbuf, xrecv, ybuf, yrecv, obuf, orecv,
    quad_s, quad_r, psum_s, psum_r, zsum_s, zsum_r, mean_s, mean_r,
    up1_s, up1_r, dn1_s, dn1_r, up2_s, up2_r, dn2_s, dn2_r,
    d_s, d_r, x_s, x_r, y_s, y_r, o_s, o_r, token, complete,
):
    s, p = lax.axis_index("snap"), lax.axis_index("space")
    z, xh, c = s // 4, (s // 2) % 2, s % 2
    y, xl = p // 2, p % 2
    x = xh * 2 + xl
    q0 = xh * 2 + c
    quad = {
        1: (device(z, x, y, 1 - c), xh * 2 + 1 - c),
        2: (device(z, x + 2, y, c), (1 - xh) * 2 + c),
        3: (device(z, x + 2, y, 1 - c), (1 - xh) * 2 + 1 - c),
    }

    def send(src, dst, ss, rs, to):
        pltpu.make_async_remote_copy(
            src_ref=src, dst_ref=dst, send_sem=ss, recv_sem=rs,
            device_id=to, device_id_type=MESH,
        ).start()

    barrier = pltpu.get_barrier_semaphore()

    def tell(sem, to):
        pl.semaphore_signal(sem, inc=1, device_id=to, device_id_type=MESH)

    above, below = device(z + 1, x, y, c), device(z - 1, x, y, c)
    partners = [quad[1][0], quad[2][0], quad[3][0]]
    partners += [device(z, x + 1, y, c), device(z, x + 3, y, c)]
    partners += [device(z, x, y - k, c) for k in range(1, NY)]
    for to in partners + [below]:
        tell(barrier, to)
    pl.when(z != NZ - 1)(lambda: tell(barrier, above))

    def row_sums(i, carry):
        block = a_ref[pl.ds(pl.multiple_of(i * LANES, LANES), LANES), :].astype(F32)
        psum[pl.ds(i, 1), :] = jnp.sum(block.T, axis=0, keepdims=True)
        return carry

    lax.fori_loop(0, 32, row_sums, 0)
    own_rows = pl.ds(pl.multiple_of(q0 * ROWS_Q, ROWS_Q), ROWS_Q)
    raw0[q0] = a_ref[own_rows, :]

    pl.semaphore_wait(barrier, len(partners) + 1 + (z + NZ - 1) // NZ)

    for j in (1, 2, 3):
        to, q = quad[j]
        send(psum.at[pl.ds(pl.multiple_of(q * 8, 8), 8)], qrecv.at[j - 1], psum_s, psum_r, to)

    def send_up(src, a):
        send(src, lo1.at[a], up1_s.at[a], up1_r.at[a], above)

    def send_down(src, a):
        send(src, hi1.at[a], dn1_s.at[a], dn1_r.at[a], below)

    send_up(a_ref.at[own_rows], q0)
    pl.when(z != 0)(lambda: send_down(a_ref.at[own_rows], q0))
    for j in (1, 2, 3):
        to, q = quad[j]
        rows = pl.ds(pl.multiple_of(q * ROWS_Q, ROWS_Q), ROWS_Q)
        send(a_ref.at[rows], raw0.at[q0], quad_s.at[j - 1], quad_r.at[j - 1], to)

    pl.when(z != 0)(lambda: pl.semaphore_wait(token, 1))
    pl.when(z != NZ - 1)(lambda: tell(token, above))

    @pl.when(z == NZ - 1)
    def _():
        for k in range(1, NZ):
            tell(complete, device(z + k, x, y, c))

    wait_for(qrecv, psum_r)
    zrecv[z] = psum[pl.ds(pl.multiple_of(q0 * 8, 8), 8), :] + qrecv[0] + qrecv[1] + qrecv[2]

    def sums_along_z():
        pl.when(z != NZ - 1)(lambda: pl.semaphore_wait(complete, 1))
        for k in range(1, NZ):
            send(zrecv.at[z], zrecv.at[z], zsum_s, zsum_r, device(z + k, x, y, c))

    sibling = quad[1][1]
    pl.when(z >= 3)(sums_along_z)
    wait_for(raw0.at[sibling], quad_r.at[0])
    send_up(raw0.at[sibling], sibling)

    @pl.when(z < 3)
    def _():
        pl.when(z != 0)(lambda: send_down(raw0.at[sibling], sibling))
        sums_along_z()
        pl.when(z == 0)(lambda: send_down(a_ref.at[own_rows], q0))

    pl.when((z == 0) | (z >= 3))(lambda: send_down(raw0.at[sibling], sibling))

    def quad_slab(j):
        q = quad[j][1]
        wait_for(raw0.at[q], quad_r.at[j - 1])
        send_up(raw0.at[q], q)
        send_down(raw0.at[q], q)

    quad_slab(2)

    wait_for(zrecv.at[pl.ds(0, NZ - 1)], zsum_r)
    mean = zrecv[0]
    for k in range(1, NZ):
        mean = mean + zrecv[k]
    mean = mean * (1.0 / SNAPS)
    mall[q0] = mean
    for j in (1, 2, 3):
        send(mall.at[q0], mall.at[q0], mean_s, mean_r, quad[j][0])
    for g in range(8):
        mcol[pl.ds(g * LANES, LANES), :] = jnp.broadcast_to(mean[g : g + 1, :], (LANES, LANES)).T

    quad_slab(3)

    def centred(ref, a):
        return (ref[a].astype(F32) - mcol[...]).astype(BF16)

    def fill_lhs(ref, a, at):
        lhs[pl.ds(at * 512 + a * LANES, LANES), :] = centred(ref, a).T

    def store_unit(g, u, tile, first=0):
        blocks = tile.reshape((4 - first), 8, 2, 8, LANES)
        for a in range(4):
            for half in range(2):
                if a < first:
                    value = jnp.zeros((8, 8, LANES), F32)
                else:
                    value = blocks[a - first, :, half]
                part[g, a % 2, (a // 2) * 2 + half, :, u] = value

    def dot(start, size, right):
        return jnp.dot(lhs[pl.ds(start, size), :], right, preferred_element_type=F32)

    groups = [("a", 3), ("a", 1)] + [("b", t) for t in (3, 2, 1, 0)] + [("c", t) for t in (3, 2, 1, 0)]
    shifts = {"a": (0, 0), "b": (0, 1), "c": (1, 2)}
    dz = {"a": (0, 0), "b": (1, 2), "c": (3, 4)}

    def make(g):
        kind, t = groups[g]
        if kind == "a":
            for u in range(2):
                store_unit(g, u, dot(0, 512, centred(raw0, t - u)))
        elif kind == "b":
            right = centred(hi1, t)
            for u in range(2):
                store_unit(g, u, dot(u * 512, 512, right))
        else:
            wait_for(lo2.at[t], up2_r.at[t])
            wait_for(hi2.at[t], dn2_r.at[t])
            fill_lhs(lo2, t, 2)
            right = centred(hi2, t)
            store_unit(g, 0, dot(512, 512, right))
            store_unit(g, 1, dot(1024 + t * LANES, 512 - t * LANES, right), t)
        send(part.at[g, 1 - c], drecv.at[g], d_s.at[g], d_r.at[g], quad[1][0])

    def x_step(g):
        wait_for(drecv.at[g], d_r.at[g])
        xbuf[g] = part[g, c] + drecv[g]
        for k in range(1, NX):
            xt = (x + k) % NX
            send(xbuf.at[g, xt], xrecv.at[g, k - 1], x_s.at[g], x_r.at[g], device(z, xt, y, c))

    def y_step(g):
        wait_for(xrecv.at[g], x_r.at[g])
        ybuf[g] = xbuf[g, x] + xrecv[g, 0] + xrecv[g, 1] + xrecv[g, 2]
        for k in range(1, NY):
            yt = (y + k) % NY
            send(ybuf.at[g, yt], yrecv.at[g, k - 1], y_s.at[g], y_r.at[g], device(z, x, yt, c))

    def o_step(g):
        wait_for(yrecv.at[g], y_r.at[g])
        total = ybuf[g, y]
        for k in range(NY - 1):
            total = total + yrecv[g, k]
        obuf[g] = total * (1.0 / ROWS)
        for u in range(2):
            shift = shifts[groups[g][0]][u]
            if shift:
                send(obuf.at[g, u], orecv.at[g, u], o_s.at[g, u], o_r.at[g, u], device(z - shift, x, y, c))

    def f_step(g):
        kind, t = groups[g]
        for u in range(2):
            if shifts[kind][u]:
                wait_for(orecv.at[g, u], o_r.at[g, u])
                total = orecv[g, u]
            else:
                total = obuf[g, u]
            d = dz[kind][u]
            col = t - u if kind == "a" else t

            def put(total=total, d=d, col=col):
                at = pl.multiple_of((4 * d + col - q0) * LANES, LANES)
                gram_ref[:, pl.ds(at, LANES)] = total

            if d == 0:
                pl.when(col >= q0)(put)
            elif d == 4:
                pl.when(col <= q0)(put)
            else:
                put()

    for a in range(4):
        fill_lhs(raw0, a, 0)
    make(0)
    make(1)
    x_step(0)
    for t in (3, 2, 1, 0):
        wait_for(lo1.at[t], up1_r.at[t])
        send(lo1.at[t], lo2.at[t], up2_s.at[t], up2_r.at[t], above)
        wait_for(hi1.at[t], dn1_r.at[t])
        send(hi1.at[t], hi2.at[t], dn2_s.at[t], dn2_r.at[t], below)
    x_step(1)
    for t in (3, 2, 1, 0):
        fill_lhs(lo1, t, 1)
    steps = {"m": make, "x": x_step, "y": y_step, "o": o_step}
    order = (
        ("m", 2), ("m", 3), ("x", 2), ("m", 4), ("x", 3), ("m", 5), ("x", 4), ("y", 0), ("x", 5), ("y", 1), ("o", 0),
        ("m", 6), ("x", 6), ("y", 2), ("o", 1), ("y", 3),
        ("m", 7), ("x", 7), ("y", 4), ("o", 2), ("y", 5), ("o", 3),
        ("m", 8), ("x", 8), ("y", 6), ("o", 4), ("o", 5), ("y", 7), ("o", 6),
        ("m", 9), ("y", 8), ("x", 9), ("o", 7), ("o", 8), ("y", 9), ("o", 9),
    )
    for kind, g in order:
        steps[kind](g)
    for g in range(GROUPS):
        f_step(g)

    wait_for(mall.at[pl.ds(0, 3)], mean_r)
    mean_ref[...] = mall[...]

    wait_for(qrecv, psum_s)
    wait_for(zrecv.at[pl.ds(0, NZ - 1)], zsum_s)
    wait_for(mall.at[pl.ds(0, 3)], mean_s)
    for j in range(3):
        wait_for(raw0.at[j], quad_s.at[j])
    for a in range(4):
        for sem in (up1_s, dn1_s, up2_s, dn2_s):
            wait_for(raw0.at[a], sem.at[a])
    for g in range(GROUPS):
        wait_for(drecv.at[g], d_s.at[g])
        wait_for(xrecv.at[g], x_s.at[g])
        wait_for(yrecv.at[g], y_s.at[g])
        for u in range(2):
            if shifts[groups[g][0]][u]:
                wait_for(orecv.at[g, u], o_s.at[g, u])


def per_device(snapshots):
    slab = lambda: pltpu.VMEM((4, ROWS_Q, LANES), BF16)
    dma = pltpu.SemaphoreType.DMA
    one = lambda: dma(())
    gram, mean = pl.pallas_call(
        kernel,
        out_shape=(
            jax.ShapeDtypeStruct((8, 17 * LANES), F32),
            jax.ShapeDtypeStruct((4, 8, LANES), F32),
        ),
        in_specs=[pl.BlockSpec(memory_space=pltpu.VMEM)],
        out_specs=(pl.BlockSpec(memory_space=pltpu.VMEM),) * 2,
        scratch_shapes=[
            slab(), slab(), slab(), slab(), slab(),
            pltpu.VMEM((3 * 512, ROWS_Q), BF16),
            pltpu.VMEM((ROWS_Q, LANES), F32),
            pltpu.VMEM((32, LANES), F32),
            pltpu.VMEM((3, 8, LANES), F32),
            pltpu.VMEM((NZ, 8, LANES), F32),
            pltpu.VMEM((4, 8, LANES), F32),
            pltpu.VMEM((GROUPS, 2, NX, NY, 2, 8, LANES), F32),
            pltpu.VMEM((GROUPS, NX, NY, 2, 8, LANES), F32),
            pltpu.VMEM((GROUPS, NX, NY, 2, 8, LANES), F32),
            pltpu.VMEM((GROUPS, NX - 1, NY, 2, 8, LANES), F32),
            pltpu.VMEM((GROUPS, NY, 2, 8, LANES), F32),
            pltpu.VMEM((GROUPS, NY - 1, 2, 8, LANES), F32),
            pltpu.VMEM((GROUPS, 2, 8, LANES), F32),
            pltpu.VMEM((GROUPS, 2, 8, LANES), F32),
            dma((3,)), dma((3,)), one(), one(), one(), one(), one(), one(),
            dma((4,)), dma((4,)), dma((4,)), dma((4,)), dma((4,)), dma((4,)), dma((4,)), dma((4,)),
            dma((GROUPS,)), dma((GROUPS,)), dma((GROUPS,)), dma((GROUPS,)),
            dma((GROUPS,)), dma((GROUPS,)), dma((GROUPS, 2)), dma((GROUPS, 2)),
            pltpu.SemaphoreType.REGULAR, pltpu.SemaphoreType.REGULAR,
        ],
        compiler_params=pltpu.CompilerParams(
            collective_id=0, has_side_effects=True, vmem_limit_bytes=48 * 1024 * 1024
        ),
    )(snapshots)
    return gram, mean.reshape(-1)


def solution(mesh):
    return jax.shard_map(
        per_device,
        mesh=mesh,
        in_specs=(P("space", "snap"),),
        out_specs=(P(("snap", "space"), None), P("space")),
        check_vma=False,
    )
```

```python
import jax
import jax.numpy as jnp
from jax import lax
from jax.experimental import pallas as pl
from jax.experimental.pallas import tpu as pltpu
from jax.sharding import PartitionSpec as P

MESH = pl.DeviceIdType.MESH
NZ, NX, NY = 8, 4, 8
LANES = 128
ROWS_Q = 1024
SNAPS = 4096
ROWS = 65536
GROUPS = 10
F32, BF16 = jnp.float32, jnp.bfloat16


def device(z, x, y, c):
    z, x, y = (z + NZ) % NZ, (x + NX) % NX, (y + NY) % NY
    return (z * 4 + (x // 2) * 2 + c, y * 2 + x % 2)


def wait_for(ref, sem):
    pltpu.make_async_copy(ref, ref, sem).wait()


def kernel(
    a_ref, gram_ref, mean_ref,
    raw0, lo1, hi1, lo2, hi2, lhs, mcol, psum, qrecv, zrecv, mall,
    part, drecv, xbuf, xrecv, ybuf, yrecv, obuf, orecv,
    quad_s, quad_r, psum_s, psum_r, zsum_s, zsum_r, mean_s, mean_r,
    up1_s, up1_r, dn1_s, dn1_r, up2_s, up2_r, dn2_s, dn2_r,
    d_s, d_r, x_s, x_r, y_s, y_r, o_s, o_r, token, complete,
):
    s, p = lax.axis_index("snap"), lax.axis_index("space")
    z, xh, c = s // 4, (s // 2) % 2, s % 2
    y, xl = p // 2, p % 2
    x = xh * 2 + xl
    q0 = xh * 2 + c
    quad = {
        1: (device(z, x, y, 1 - c), xh * 2 + 1 - c),
        2: (device(z, x + 2, y, c), (1 - xh) * 2 + c),
        3: (device(z, x + 2, y, 1 - c), (1 - xh) * 2 + 1 - c),
    }

    def send(src, dst, ss, rs, to):
        pltpu.make_async_remote_copy(
            src_ref=src, dst_ref=dst, send_sem=ss, recv_sem=rs,
            device_id=to, device_id_type=MESH,
        ).start()

    barrier = pltpu.get_barrier_semaphore()

    def tell(sem, to):
        pl.semaphore_signal(sem, inc=1, device_id=to, device_id_type=MESH)

    above, below = device(z + 1, x, y, c), device(z - 1, x, y, c)
    partners = [quad[1][0], quad[2][0], quad[3][0]]
    partners += [device(z, x + 1, y, c), device(z, x + 3, y, c)]
    partners += [device(z, x, y - k, c) for k in range(1, NY)]
    for to in partners + [below]:
        tell(barrier, to)
    pl.when(z != NZ - 1)(lambda: tell(barrier, above))

    def row_sums(i, carry):
        block = a_ref[pl.ds(pl.multiple_of(i * LANES, LANES), LANES), :].astype(F32)
        psum[pl.ds(i, 1), :] = jnp.sum(block.T, axis=0, keepdims=True)
        return carry

    lax.fori_loop(0, 32, row_sums, 0)
    own_rows = pl.ds(pl.multiple_of(q0 * ROWS_Q, ROWS_Q), ROWS_Q)
    raw0[q0] = a_ref[own_rows, :]

    pl.semaphore_wait(barrier, len(partners) + 1 + (z + NZ - 1) // NZ)

    for j in (1, 2, 3):
        to, q = quad[j]
        send(psum.at[pl.ds(pl.multiple_of(q * 8, 8), 8)], qrecv.at[j - 1], psum_s, psum_r, to)

    def send_up(src, a):
        send(src, lo1.at[a], up1_s.at[a], up1_r.at[a], above)

    def send_down(src, a):
        send(src, hi1.at[a], dn1_s.at[a], dn1_r.at[a], below)

    send_up(a_ref.at[own_rows], q0)
    pl.when(z != 0)(lambda: send_down(a_ref.at[own_rows], q0))
    for j in (1, 2, 3):
        to, q = quad[j]
        rows = pl.ds(pl.multiple_of(q * ROWS_Q, ROWS_Q), ROWS_Q)
        send(a_ref.at[rows], raw0.at[q0], quad_s.at[j - 1], quad_r.at[j - 1], to)

    pl.when(z != 0)(lambda: pl.semaphore_wait(token, 1))
    pl.when(z != NZ - 1)(lambda: tell(token, above))

    @pl.when(z == NZ - 1)
    def _():
        for k in range(1, NZ):
            tell(complete, device(z + k, x, y, c))

    wait_for(qrecv, psum_r)
    zrecv[z] = psum[pl.ds(pl.multiple_of(q0 * 8, 8), 8), :] + qrecv[0] + qrecv[1] + qrecv[2]

    def sums_along_z():
        pl.when(z != NZ - 1)(lambda: pl.semaphore_wait(complete, 1))
        for k in range(1, NZ):
            send(zrecv.at[z], zrecv.at[z], zsum_s, zsum_r, device(z + k, x, y, c))

    sibling = quad[1][1]
    pl.when(z >= 3)(sums_along_z)
    wait_for(raw0.at[sibling], quad_r.at[0])
    send_up(raw0.at[sibling], sibling)

    @pl.when(z < 3)
    def _():
        pl.when(z != 0)(lambda: send_down(raw0.at[sibling], sibling))
        sums_along_z()
        pl.when(z == 0)(lambda: send_down(a_ref.at[own_rows], q0))

    pl.when((z == 0) | (z >= 3))(lambda: send_down(raw0.at[sibling], sibling))

    def quad_slab(j):
        q = quad[j][1]
        wait_for(raw0.at[q], quad_r.at[j - 1])
        send_up(raw0.at[q], q)
        send_down(raw0.at[q], q)

    quad_slab(2)

    wait_for(zrecv.at[pl.ds(0, NZ - 1)], zsum_r)
    mean = zrecv[0]
    for k in range(1, NZ):
        mean = mean + zrecv[k]
    mean = mean * (1.0 / SNAPS)
    mall[q0] = mean
    for j in (1, 2, 3):
        send(mall.at[q0], mall.at[q0], mean_s, mean_r, quad[j][0])
    for g in range(8):
        mcol[pl.ds(g * LANES, LANES), :] = jnp.broadcast_to(mean[g : g + 1, :], (LANES, LANES)).T

    quad_slab(3)

    def centred(ref, a):
        return (ref[a].astype(F32) - mcol[...]).astype(BF16)

    def fill_lhs(ref, a, at):
        lhs[pl.ds(at * 512 + a * LANES, LANES), :] = centred(ref, a).T

    def store_unit(g, u, tile, first=0):
        blocks = tile.reshape((4 - first), 8, 2, 8, LANES)
        for a in range(4):
            for half in range(2):
                if a < first:
                    value = jnp.zeros((8, 8, LANES), F32)
                else:
                    value = blocks[a - first, :, half]
                part[g, u, a % 2, (a // 2) * 2 + half] = value

    def dot(start, size, right):
        return jnp.dot(lhs[pl.ds(start, size), :], right, preferred_element_type=F32)

    groups = [("a", 3), ("a", 1)] + [("b", t) for t in (3, 2, 1, 0)] + [("c", t) for t in (3, 2, 1, 0)]
    shifts = {"a": (0, 0), "b": (0, 1), "c": (1, 2)}
    dz = {"a": (0, 0), "b": (1, 2), "c": (3, 4)}

    def swap(g, u):
        send(part.at[g, u, 1 - c], drecv.at[g, u], d_s.at[g, u], d_r.at[g, u], quad[1][0])

    def make(g):
        kind, t = groups[g]
        if kind == "a":
            for u in range(2):
                store_unit(g, u, dot(0, 512, centred(raw0, t - u)))
                swap(g, u)
        elif kind == "b":
            right = centred(hi1, t)
            for u in range(2):
                store_unit(g, u, dot(u * 512, 512, right))
                swap(g, u)
        else:
            wait_for(hi2.at[t], dn2_r.at[t])
            right = centred(hi2, t)
            store_unit(g, 0, dot(512, 512, right))
            swap(g, 0)
            wait_for(lo2.at[t], up2_r.at[t])
            fill_lhs(lo2, t, 2)
            store_unit(g, 1, dot(1024 + t * LANES, 512 - t * LANES, right), t)
            swap(g, 1)

    def x_step(g):
        for u in range(2):
            wait_for(drecv.at[g, u], d_r.at[g, u])
            xbuf[g, u] = part[g, u, c] + drecv[g, u]
            for k in (2, 1, 3):
                xt = (x + k) % NX
                send(xbuf.at[g, u, xt], xrecv.at[g, u, k - 1], x_s.at[g, u], x_r.at[g, u], device(z, xt, y, c))

    def y_step(g):
        for u in range(2):
            wait_for(xrecv.at[g, u], x_r.at[g, u])
            ybuf[g, :, u] = xbuf[g, u, x] + xrecv[g, u, 0] + xrecv[g, u, 1] + xrecv[g, u, 2]
        for k in (4, 3, 5, 2, 6, 1, 7):
            yt = (y + k) % NY
            send(ybuf.at[g, yt], yrecv.at[g, k - 1], y_s.at[g], y_r.at[g], device(z, x, yt, c))

    def o_step(g):
        wait_for(yrecv.at[g], y_r.at[g])
        total = ybuf[g, y]
        for k in range(NY - 1):
            total = total + yrecv[g, k]
        obuf[g] = total * (1.0 / ROWS)
        for u in range(2):
            shift = shifts[groups[g][0]][u]
            if shift:
                send(obuf.at[g, u], orecv.at[g, u], o_s.at[g, u], o_r.at[g, u], device(z - shift, x, y, c))

    def f_step(g):
        kind, t = groups[g]
        for u in range(2):
            if shifts[kind][u]:
                wait_for(orecv.at[g, u], o_r.at[g, u])
                total = orecv[g, u]
            else:
                total = obuf[g, u]
            d = dz[kind][u]
            col = t - u if kind == "a" else t

            def put(total=total, d=d, col=col):
                at = pl.multiple_of((4 * d + col - q0) * LANES, LANES)
                gram_ref[:, pl.ds(at, LANES)] = total

            if d == 0:
                pl.when(col >= q0)(put)
            elif d == 4:
                pl.when(col <= q0)(put)
            else:
                put()

    for a in range(4):
        fill_lhs(raw0, a, 0)
    make(0)
    make(1)
    x_step(0)
    for t in (3, 2, 1, 0):
        wait_for(lo1.at[t], up1_r.at[t])
        send(lo1.at[t], lo2.at[t], up2_s.at[t], up2_r.at[t], above)
        wait_for(hi1.at[t], dn1_r.at[t])
        send(hi1.at[t], hi2.at[t], dn2_s.at[t], dn2_r.at[t], below)
    x_step(1)
    for t in (3, 2, 1, 0):
        fill_lhs(lo1, t, 1)
    steps = {"m": make, "x": x_step, "y": y_step, "o": o_step}
    order = (("m", 2), ("m", 3), ("x", 2), ("m", 4), ("x", 3), ("m", 5), ("x", 4), ("x", 5), ("y", 0), ("y", 1), ("m", 6), ("x", 6), ("o", 0), ("y", 2), ("o", 1), ("m", 7), ("x", 7), ("y", 3), ("y", 4), ("o", 2), ("m", 8), ("x", 8), ("y", 5), ("y", 6), ("o", 3), ("o", 4), ("m", 9), ("x", 9), ("y", 7), ("y", 8), ("o", 5), ("o", 6), ("o", 7), ("o", 8), ("y", 9), ("o", 9),)
    for kind, g in order:
        steps[kind](g)
    for g in range(GROUPS):
        f_step(g)

    wait_for(mall.at[pl.ds(0, 3)], mean_r)
    mean_ref[...] = mall[...]

    wait_for(qrecv, psum_s)
    wait_for(zrecv.at[pl.ds(0, NZ - 1)], zsum_s)
    wait_for(mall.at[pl.ds(0, 3)], mean_s)
    for j in range(3):
        wait_for(raw0.at[j], quad_s.at[j])
    for a in range(4):
        for sem in (up1_s, dn1_s, up2_s, dn2_s):
            wait_for(raw0.at[a], sem.at[a])
    for g in range(GROUPS):
        wait_for(yrecv.at[g], y_s.at[g])
        for u in range(2):
            wait_for(drecv.at[g, u], d_s.at[g, u])
            wait_for(xrecv.at[g, u], x_s.at[g, u])
            if shifts[groups[g][0]][u]:
                wait_for(orecv.at[g, u], o_s.at[g, u])


def per_device(snapshots):
    slab = lambda: pltpu.VMEM((4, ROWS_Q, LANES), BF16)
    dma = pltpu.SemaphoreType.DMA
    one = lambda: dma(())
    gram, mean = pl.pallas_call(
        kernel,
        out_shape=(
            jax.ShapeDtypeStruct((8, 17 * LANES), F32),
            jax.ShapeDtypeStruct((4, 8, LANES), F32),
        ),
        in_specs=[pl.BlockSpec(memory_space=pltpu.VMEM)],
        out_specs=(pl.BlockSpec(memory_space=pltpu.VMEM),) * 2,
        scratch_shapes=[
            slab(), slab(), slab(), slab(), slab(),
            pltpu.VMEM((3 * 512, ROWS_Q), BF16),
            pltpu.VMEM((ROWS_Q, LANES), F32),
            pltpu.VMEM((32, LANES), F32),
            pltpu.VMEM((3, 8, LANES), F32),
            pltpu.VMEM((NZ, 8, LANES), F32),
            pltpu.VMEM((4, 8, LANES), F32),
            pltpu.VMEM((GROUPS, 2, 2, NX, NY, 8, LANES), F32),
            pltpu.VMEM((GROUPS, 2, NX, NY, 8, LANES), F32),
            pltpu.VMEM((GROUPS, 2, NX, NY, 8, LANES), F32),
            pltpu.VMEM((GROUPS, 2, NX - 1, NY, 8, LANES), F32),
            pltpu.VMEM((GROUPS, NY, 2, 8, LANES), F32),
            pltpu.VMEM((GROUPS, NY - 1, 2, 8, LANES), F32),
            pltpu.VMEM((GROUPS, 2, 8, LANES), F32),
            pltpu.VMEM((GROUPS, 2, 8, LANES), F32),
            dma((3,)), dma((3,)), one(), one(), one(), one(), one(), one(),
            dma((4,)), dma((4,)), dma((4,)), dma((4,)), dma((4,)), dma((4,)), dma((4,)), dma((4,)),
            dma((GROUPS, 2)), dma((GROUPS, 2)), dma((GROUPS, 2)), dma((GROUPS, 2)),
            dma((GROUPS,)), dma((GROUPS,)), dma((GROUPS, 2)), dma((GROUPS, 2)),
            pltpu.SemaphoreType.REGULAR, pltpu.SemaphoreType.REGULAR,
        ],
        compiler_params=pltpu.CompilerParams(
            collective_id=0, has_side_effects=True, vmem_limit_bytes=48 * 1024 * 1024
        ),
    )(snapshots)
    return gram, mean.reshape(-1)


def solution(mesh):
    return jax.shard_map(
        per_device,
        mesh=mesh,
        in_specs=(P("space", "snap"),),
        out_specs=(P(("snap", "space"), None), P("space")),
        check_vma=False,
    )
```

```python
import jax
import jax.numpy as jnp
from jax import lax
from jax.experimental import pallas as pl
from jax.experimental.pallas import tpu as pltpu
from jax.sharding import PartitionSpec as P

MESH = pl.DeviceIdType.MESH
NZ, NX, NY = 8, 4, 8
LANES = 128
ROWS_Q = 1024
SNAPS = 4096
ROWS = 65536
GROUPS = 10
F32, BF16 = jnp.float32, jnp.bfloat16


def device(z, x, y, c):
    z, x, y = (z + NZ) % NZ, (x + NX) % NX, (y + NY) % NY
    return (z * 4 + (x // 2) * 2 + c, y * 2 + x % 2)


def wait_for(ref, sem):
    pltpu.make_async_copy(ref, ref, sem).wait()


def kernel(
    a_ref, gram_ref, mean_ref,
    raw0, lo1, hi1, lo2, hi2, lhs, mcol, psum, qrecv, zrecv, mall,
    part, drecv, xbuf, xrecv, ybuf, yrecv, obuf, orecv,
    quad_s, quad_r, psum_s, psum_r, zsum_s, zsum_r, mean_s, mean_r,
    up1_s, up1_r, dn1_s, dn1_r, up2_s, up2_r, dn2_s, dn2_r,
    d_s, d_r, x_s, x_r, y_s, y_r, o_s, o_r, token, complete,
):
    s, p = lax.axis_index("snap"), lax.axis_index("space")
    z, xh, c = s // 4, (s // 2) % 2, s % 2
    y, xl = p // 2, p % 2
    x = xh * 2 + xl
    q0 = xh * 2 + c
    quad = {
        1: (device(z, x, y, 1 - c), xh * 2 + 1 - c),
        2: (device(z, x + 2, y, c), (1 - xh) * 2 + c),
        3: (device(z, x + 2, y, 1 - c), (1 - xh) * 2 + 1 - c),
    }

    def send(src, dst, ss, rs, to):
        pltpu.make_async_remote_copy(
            src_ref=src, dst_ref=dst, send_sem=ss, recv_sem=rs,
            device_id=to, device_id_type=MESH,
        ).start()

    barrier = pltpu.get_barrier_semaphore()

    def tell(sem, to):
        pl.semaphore_signal(sem, inc=1, device_id=to, device_id_type=MESH)

    above, below = device(z + 1, x, y, c), device(z - 1, x, y, c)
    partners = [quad[1][0], quad[2][0], quad[3][0]]
    partners += [device(z, x + 1, y, c), device(z, x + 3, y, c)]
    partners += [device(z, x, y - k, c) for k in range(1, NY)]
    for to in partners + [below]:
        tell(barrier, to)
    pl.when(z != NZ - 1)(lambda: tell(barrier, above))

    def row_sums(i, carry):
        block = a_ref[pl.ds(pl.multiple_of(i * LANES, LANES), LANES), :].astype(F32)
        psum[pl.ds(i, 1), :] = jnp.sum(block.T, axis=0, keepdims=True)
        return carry

    lax.fori_loop(0, 32, row_sums, 0)
    own_rows = pl.ds(pl.multiple_of(q0 * ROWS_Q, ROWS_Q), ROWS_Q)
    raw0[q0] = a_ref[own_rows, :]

    pl.semaphore_wait(barrier, len(partners) + 1 + (z + NZ - 1) // NZ)

    for j in (1, 2, 3):
        to, q = quad[j]
        send(psum.at[pl.ds(pl.multiple_of(q * 8, 8), 8)], qrecv.at[j - 1], psum_s, psum_r, to)

    def send_up(src, a):
        send(src, lo1.at[a], up1_s.at[a], up1_r.at[a], above)

    def send_down(src, a):
        send(src, hi1.at[a], dn1_s.at[a], dn1_r.at[a], below)

    send_up(a_ref.at[own_rows], q0)
    pl.when(z != 0)(lambda: send_down(a_ref.at[own_rows], q0))
    for j in (1, 2, 3):
        to, q = quad[j]
        rows = pl.ds(pl.multiple_of(q * ROWS_Q, ROWS_Q), ROWS_Q)
        send(a_ref.at[rows], raw0.at[q0], quad_s.at[j - 1], quad_r.at[j - 1], to)

    pl.when(z != 0)(lambda: pl.semaphore_wait(token, 1))
    pl.when(z != NZ - 1)(lambda: tell(token, above))

    @pl.when(z == NZ - 1)
    def _():
        for k in range(1, NZ):
            tell(complete, device(z + k, x, y, c))

    wait_for(qrecv, psum_r)
    zrecv[z] = psum[pl.ds(pl.multiple_of(q0 * 8, 8), 8), :] + qrecv[0] + qrecv[1] + qrecv[2]

    def sums_along_z():
        pl.when(z != NZ - 1)(lambda: pl.semaphore_wait(complete, 1))
        for k in range(1, NZ):
            send(zrecv.at[z], zrecv.at[z], zsum_s, zsum_r, device(z + k, x, y, c))

    sibling = quad[1][1]
    pl.when(z >= 3)(sums_along_z)
    wait_for(raw0.at[sibling], quad_r.at[0])
    send_up(raw0.at[sibling], sibling)

    @pl.when(z < 3)
    def _():
        pl.when(z != 0)(lambda: send_down(raw0.at[sibling], sibling))
        sums_along_z()
        pl.when(z == 0)(lambda: send_down(a_ref.at[own_rows], q0))

    pl.when((z == 0) | (z >= 3))(lambda: send_down(raw0.at[sibling], sibling))

    def quad_slab(j):
        q = quad[j][1]
        wait_for(raw0.at[q], quad_r.at[j - 1])
        send_up(raw0.at[q], q)
        send_down(raw0.at[q], q)

    quad_slab(2)

    wait_for(zrecv.at[pl.ds(0, NZ - 1)], zsum_r)
    mean = zrecv[0]
    for k in range(1, NZ):
        mean = mean + zrecv[k]
    mean = mean * (1.0 / SNAPS)
    mall[q0] = mean
    for j in (1, 2, 3):
        send(mall.at[q0], mall.at[q0], mean_s, mean_r, quad[j][0])
    for g in range(8):
        mcol[pl.ds(g * LANES, LANES), :] = jnp.broadcast_to(mean[g : g + 1, :], (LANES, LANES)).T

    quad_slab(3)

    def centred(ref, a):
        return (ref[a].astype(F32) - mcol[...]).astype(BF16)

    def fill_lhs(ref, a, at):
        lhs[pl.ds(at * 512 + a * LANES, LANES), :] = centred(ref, a).T

    def store_unit(g, u, tile, first=0):
        blocks = tile.reshape((4 - first), 8, 2, 8, LANES)
        for a in range(4):
            for half in range(2):
                if a < first:
                    value = jnp.zeros((8, 8, LANES), F32)
                else:
                    value = blocks[a - first, :, half]
                part[g, u, a % 2, (a // 2) * 2 + half] = value

    def dot(start, size, right):
        return jnp.dot(lhs[pl.ds(start, size), :], right, preferred_element_type=F32)

    groups = [("a", 3), ("a", 1)] + [("b", t) for t in (3, 2, 1, 0)] + [("c", t) for t in (3, 2, 1, 0)]
    shifts = {"a": (0, 0), "b": (0, 1), "c": (1, 2)}
    dz = {"a": (0, 0), "b": (1, 2), "c": (3, 4)}

    def swap(g, u):
        send(part.at[g, u, 1 - c], drecv.at[g, u], d_s.at[g, u], d_r.at[g, u], quad[1][0])

    def make(g):
        kind, t = groups[g]
        if kind == "a":
            for u in range(2):
                store_unit(g, u, dot(0, 512, centred(raw0, t - u)))
                swap(g, u)
        elif kind == "b":
            right = centred(hi1, t)
            for u in range(2):
                store_unit(g, u, dot(u * 512, 512, right))
                swap(g, u)
        else:
            wait_for(hi2.at[t], dn2_r.at[t])
            right = centred(hi2, t)
            store_unit(g, 0, dot(512, 512, right))
            swap(g, 0)
            wait_for(lo2.at[t], up2_r.at[t])
            fill_lhs(lo2, t, 2)
            store_unit(g, 1, dot(1024 + t * LANES, 512 - t * LANES, right), t)
            swap(g, 1)

    def where_used(g, u, a, run):
        kind, t = groups[g]
        col = t - u if kind == "a" else t
        if dz[kind][u] == 0 and col < 3:
            pl.when(a <= col)(run)
        elif dz[kind][u] == 4 and col > 0:
            pl.when(a >= col)(run)
        else:
            run()

    def x_step(g):
        for u in range(2):
            wait_for(drecv.at[g, u], d_r.at[g, u])
            xbuf[g, u] = part[g, u, c] + drecv[g, u]
            for k in (2, 1, 3):
                xt = (x + k) % NX

                def go(k=k, xt=xt, u=u):
                    send(
                        xbuf.at[g, u, xt], xrecv.at[g, u, k - 1],
                        x_s.at[g, u, k - 1], x_r.at[g, u], device(z, xt, y, c),
                    )

                where_used(g, u, (xt // 2) * 2 + c, go)

    def y_step(g):
        for u in range(2):

            def add(u=u):
                wait_for(xrecv.at[g, u], x_r.at[g, u])
                ybuf[g, :, u] = xbuf[g, u, x] + xrecv[g, u, 0] + xrecv[g, u, 1] + xrecv[g, u, 2]

            where_used(g, u, q0, add)
        for k in (4, 3, 5, 2, 6, 1, 7):
            yt = (y + k) % NY
            send(ybuf.at[g, yt], yrecv.at[g, k - 1], y_s.at[g], y_r.at[g], device(z, x, yt, c))

    def o_step(g):
        wait_for(yrecv.at[g], y_r.at[g])
        total = ybuf[g, y]
        for k in range(NY - 1):
            total = total + yrecv[g, k]
        obuf[g] = total * (1.0 / ROWS)
        for u in range(2):
            shift = shifts[groups[g][0]][u]
            if shift:
                send(obuf.at[g, u], orecv.at[g, u], o_s.at[g, u], o_r.at[g, u], device(z - shift, x, y, c))

    def f_step(g):
        kind, t = groups[g]
        for u in range(2):
            if shifts[kind][u]:
                wait_for(orecv.at[g, u], o_r.at[g, u])
                total = orecv[g, u]
            else:
                total = obuf[g, u]
            d = dz[kind][u]
            col = t - u if kind == "a" else t

            def put(total=total, d=d, col=col):
                at = pl.multiple_of((4 * d + col - q0) * LANES, LANES)
                gram_ref[:, pl.ds(at, LANES)] = total

            if d == 0:
                pl.when(col >= q0)(put)
            elif d == 4:
                pl.when(col <= q0)(put)
            else:
                put()

    for a in range(4):
        fill_lhs(raw0, a, 0)
    make(0)
    make(1)
    x_step(0)
    for t in (3, 2, 1, 0):
        wait_for(lo1.at[t], up1_r.at[t])
        send(lo1.at[t], lo2.at[t], up2_s.at[t], up2_r.at[t], above)
        wait_for(hi1.at[t], dn1_r.at[t])
        send(hi1.at[t], hi2.at[t], dn2_s.at[t], dn2_r.at[t], below)
    x_step(1)
    for t in (3, 2, 1, 0):
        fill_lhs(lo1, t, 1)
    steps = {"m": make, "x": x_step, "y": y_step, "o": o_step}
    order = (("m", 2), ("m", 3), ("x", 2), ("m", 4), ("x", 3), ("m", 5), ("x", 4), ("x", 5), ("y", 0), ("y", 1), ("m", 6), ("x", 6), ("o", 0), ("y", 2), ("o", 1), ("m", 7), ("x", 7), ("y", 3), ("y", 4), ("o", 2), ("m", 8), ("x", 8), ("y", 5), ("y", 6), ("o", 3), ("o", 4), ("m", 9), ("x", 9), ("y", 7), ("y", 8), ("o", 5), ("o", 6), ("o", 7), ("o", 8), ("y", 9), ("o", 9),)
    for kind, g in order:
        steps[kind](g)
    for g in range(GROUPS):
        f_step(g)

    wait_for(mall.at[pl.ds(0, 3)], mean_r)
    mean_ref[...] = mall[...]

    wait_for(qrecv, psum_s)
    wait_for(zrecv.at[pl.ds(0, NZ - 1)], zsum_s)
    wait_for(mall.at[pl.ds(0, 3)], mean_s)
    for j in range(3):
        wait_for(raw0.at[j], quad_s.at[j])
    for a in range(4):
        for sem in (up1_s, dn1_s, up2_s, dn2_s):
            wait_for(raw0.at[a], sem.at[a])
    for g in range(GROUPS):
        wait_for(yrecv.at[g], y_s.at[g])
        for u in range(2):
            wait_for(drecv.at[g, u], d_s.at[g, u])
            for k in range(1, NX):
                left = lambda: wait_for(xrecv.at[g, u, 0], x_s.at[g, u, k - 1])
                where_used(g, u, (((x + k) % NX) // 2) * 2 + c, left)
            if shifts[groups[g][0]][u]:
                wait_for(orecv.at[g, u], o_s.at[g, u])


def per_device(snapshots):
    slab = lambda: pltpu.VMEM((4, ROWS_Q, LANES), BF16)
    dma = pltpu.SemaphoreType.DMA
    one = lambda: dma(())
    gram, mean = pl.pallas_call(
        kernel,
        out_shape=(
            jax.ShapeDtypeStruct((8, 17 * LANES), F32),
            jax.ShapeDtypeStruct((4, 8, LANES), F32),
        ),
        in_specs=[pl.BlockSpec(memory_space=pltpu.VMEM)],
        out_specs=(pl.BlockSpec(memory_space=pltpu.VMEM),) * 2,
        scratch_shapes=[
            slab(), slab(), slab(), slab(), slab(),
            pltpu.VMEM((3 * 512, ROWS_Q), BF16),
            pltpu.VMEM((ROWS_Q, LANES), F32),
            pltpu.VMEM((32, LANES), F32),
            pltpu.VMEM((3, 8, LANES), F32),
            pltpu.VMEM((NZ, 8, LANES), F32),
            pltpu.VMEM((4, 8, LANES), F32),
            pltpu.VMEM((GROUPS, 2, 2, NX, NY, 8, LANES), F32),
            pltpu.VMEM((GROUPS, 2, NX, NY, 8, LANES), F32),
            pltpu.VMEM((GROUPS, 2, NX, NY, 8, LANES), F32),
            pltpu.VMEM((GROUPS, 2, NX - 1, NY, 8, LANES), F32),
            pltpu.VMEM((GROUPS, NY, 2, 8, LANES), F32),
            pltpu.VMEM((GROUPS, NY - 1, 2, 8, LANES), F32),
            pltpu.VMEM((GROUPS, 2, 8, LANES), F32),
            pltpu.VMEM((GROUPS, 2, 8, LANES), F32),
            dma((3,)), dma((3,)), one(), one(), one(), one(), one(), one(),
            dma((4,)), dma((4,)), dma((4,)), dma((4,)), dma((4,)), dma((4,)), dma((4,)), dma((4,)),
            dma((GROUPS, 2)), dma((GROUPS, 2)), dma((GROUPS, 2, NX - 1)), dma((GROUPS, 2)),
            dma((GROUPS,)), dma((GROUPS,)), dma((GROUPS, 2)), dma((GROUPS, 2)),
            pltpu.SemaphoreType.REGULAR, pltpu.SemaphoreType.REGULAR,
        ],
        compiler_params=pltpu.CompilerParams(
            collective_id=0, has_side_effects=True, vmem_limit_bytes=48 * 1024 * 1024
        ),
    )(snapshots)
    return gram, mean.reshape(-1)


def solution(mesh):
    return jax.shard_map(
        per_device,
        mesh=mesh,
        in_specs=(P("space", "snap"),),
        out_specs=(P(("snap", "space"), None), P("space")),
        check_vma=False,
    )
```
